32 devices in a mesh: tm: 8 (over y, x, core), space: 4 (over z).
Axes of the slice: x: 2, y: 2, z: 4, core: 2. Of those that a mesh axis runs over, the one named last changes fastest.
Arguments:
- previous_end: float32 [8, 16, 256, 256], P('tm', 'space'), may hold values from -6 to 6
- source: float32 [8, 16, 256, 256], P('tm', 'space'), may hold values from -4 to 4
- rate: float32 [16, 256, 256], P('space'), may hold values from 0.05 to 0.8
Outputs:
- fine_nodes: float32 [8, 2, 16, 256, 256], P('tm', None, 'space')
The draws below stay inside these ranges and needn't reach their ends.
All inputs are finite; a program needn't handle non-finite values.
Results may differ from the reference program's by a relative error of at most 0.00026.
Values sent between devices are 32-bit elements; how exact they have to be, the bound alone decides.
A program may use at most 128 MiB of HBM per device.

```python
import math
import jax
import jax.numpy as jnp
from jax import lax

NX = 256
NY = 256
TIME = 8
NZ = 16


def levels(key, dims, split, smallest, high):
    factor_of = 1.0
    for axis_at, shards_of in split:
        steps = jax.random.uniform(jax.random.fold_in(jax.random.fold_in(key, 6), axis_at), (shards_of,), jnp.float32, smallest / len(split), high / len(split))
        factor_of = factor_of * jnp.repeat(jnp.exp(steps), dims[axis_at] // shards_of).reshape((-1,) + (1,) * (len(dims) - 1 - axis_at))
    return factor_of


def scatter_about(rng, shape, spread, reach, cuts=(), held_as=jnp.bfloat16):
    drawn = jax.random.normal(rng, shape, jnp.float32) * spread
    if len(cuts) > 0:
        drawn = levels(rng, shape, cuts, -0.22, 0.18) * drawn
    return jnp.clip(drawn, min=-reach, max=reach).astype(held_as)


def setup_inputs(seed: int = 0) -> dict:
    splits = jax.random.split(jax.random.key(seed), 4)
    return {
        "previous_end": scatter_about(splits[0], (TIME, NZ, NX, NY), 1.0, 6.0, ((0, 8), (1, 4)), jnp.float32),
        "source": scatter_about(splits[1], (TIME, NZ, NX, NY), 0.5, 4.0, ((0, 8), (1, 4)), jnp.float32),
        "rate": jnp.clip(jnp.exp(math.log(0.8) - 2.7725887 * jax.random.uniform(splits[2], (NZ, NX, NY), jnp.float32) ** levels(splits[2], (NZ, NX, NY), ((0, 4),), -0.2, 0.2)), 0.05, 0.8),
    }


diffusion = 0.1
speed_z = 0.4
speed_x = 0.3
speed_y = 0.2
weights_one = (5.0 / 24.0, 1.0 / 3.0, -1.0 / 24.0)
weights_two = (-1.0 / 24.0, 1.0 / 3.0, 5.0 / 24.0)


def tendency(padded, rate_field, source_term, spacing):
    middle = padded[..., 1:-1, :, :]
    upper_z = padded[..., 2:, :, :]
    lower_z = padded[..., :-2, :, :]
    plus_x = jnp.roll(middle, -1, axis=-2)
    minus_x = jnp.roll(middle, 1, axis=-2)
    plus_y = jnp.roll(middle, -1, axis=-1)
    minus_y = jnp.roll(middle, 1, axis=-1)
    laplacian = (upper_z + lower_z + plus_x + minus_x + plus_y + minus_y - 6.0 * middle) / (spacing * spacing)
    transport = (speed_z * (upper_z - lower_z) + speed_x * (plus_x - minus_x) + speed_y * (plus_y - minus_y)) / (2.0 * spacing)
    return diffusion * laplacian - transport + rate_field * middle / (1.0 + middle * middle) + source_term


def pad_depth(field, width):
    return jnp.pad(field, [(0, 0)] * (field.ndim - 3) + [(width, width), (0, 0), (0, 0)])


def restrict(field):
    count_z, count_x, count_y = field.shape[-3:]
    blocks = field.reshape(field.shape[:-3] + (count_z // 2, 2, count_x // 2, 2, count_y // 2, 2))
    return jnp.mean(blocks, axis=(-5, -3, -1))


def inject(coarse):
    return jnp.repeat(jnp.repeat(jnp.repeat(coarse, 2, axis=-3), 2, axis=-2), 2, axis=-1)


def reference(previous_end, source, rate):
    restart = previous_end[-1]
    restart_c = restrict(restart)
    rate_c = restrict(rate)
    sources_c = lax.map(restrict, source)

    def turn(start, source_c):
        first = start + 0.5 * tendency(pad_depth(start, 1), rate_c, source_c, 2.0)
        second = first + 0.5 * tendency(pad_depth(first, 1), rate_c, source_c, 2.0)
        return second, (start, first, second)

    last_value, chained = lax.scan(turn, restart_c, sources_c)
    starts, firsts, seconds = chained

    def per_rank(items):
        warm, source_r, start, first, second = items
        warm_c = restrict(warm)
        guess = jnp.stack([restart + inject(start - restart_c), warm + inject(first - warm_c), warm + inject(second - warm_c)])
        images = tendency(pad_depth(guess, 1), rate, source_r, 1.0)
        node_one = guess[0] + (weights_one[0] * images[0] + weights_one[1] * images[1] + weights_one[2] * images[2])
        again = tendency(pad_depth(node_one, 1), rate, source_r, 1.0)
        node_two = node_one + 0.5 * (again - images[1]) + (weights_two[0] * images[0] + weights_two[1] * images[1] + weights_two[2] * images[2])
        return jnp.stack([node_one, node_two])

    return lax.map(per_rank, (previous_end, source, starts, firsts, seconds))
```

```python
import functools

import jax
import jax.numpy as jnp
from jax import lax
from jax.experimental import pallas as pl
from jax.experimental.pallas import tpu as pltpu
from jax.sharding import PartitionSpec as P

diffusion = 0.1
speed_z = 0.4
speed_x = 0.3
speed_y = 0.2
weights_one = (5.0 / 24.0, 1.0 / 3.0, -1.0 / 24.0)
weights_two = (-1.0 / 24.0, 1.0 / 3.0, 5.0 / 24.0)


def tendency(padded, rate_field, source_term, spacing):
    middle = padded[..., 1:-1, :, :]
    upper_z = padded[..., 2:, :, :]
    lower_z = padded[..., :-2, :, :]
    plus_x = jnp.roll(middle, -1, axis=-2)
    minus_x = jnp.roll(middle, 1, axis=-2)
    plus_y = jnp.roll(middle, -1, axis=-1)
    minus_y = jnp.roll(middle, 1, axis=-1)
    laplacian = (upper_z + lower_z + plus_x + minus_x + plus_y + minus_y - 6.0 * middle) / (
        spacing * spacing
    )
    transport = (
        speed_z * (upper_z - lower_z) + speed_x * (plus_x - minus_x) + speed_y * (plus_y - minus_y)
    ) / (2.0 * spacing)
    return (
        diffusion * laplacian
        - transport
        + rate_field * middle / (1.0 + middle * middle)
        + source_term
    )


def pair_table(count):
    fine_index = jnp.arange(count, dtype=jnp.int32)[:, None]
    coarse_index = jnp.arange(count // 2, dtype=jnp.int32)[None, :]
    return (fine_index // 2 == coarse_index).astype(jnp.float32)


def restrict(field):
    count_z, count_x, count_y = field.shape[-3:]
    paired = field.reshape(field.shape[:-3] + (count_z // 2, 2, count_x, count_y))
    summed_z = paired[..., 0, :, :] + paired[..., 1, :, :]
    summed_y = jnp.einsum(
        "...xy,yb->...xb", summed_z, pair_table(count_y), precision=lax.Precision.HIGHEST
    )
    summed_x = jnp.einsum(
        "...xb,xa->...ab", summed_y, pair_table(count_x), precision=lax.Precision.HIGHEST
    )
    return 0.125 * summed_x


def inject(coarse):
    count_x, count_y = coarse.shape[-2:]
    along_y = jnp.einsum(
        "...ab,yb->...ay", coarse, pair_table(2 * count_y), precision=lax.Precision.HIGHEST
    )
    along_x = jnp.einsum(
        "...ay,xa->...xy", along_y, pair_table(2 * count_x), precision=lax.Precision.HIGHEST
    )
    return along_x


MESH = pl.DeviceIdType.MESH


def coarse_tendency(middle, upper_z, lower_z, rate_field, source_term):
    flow = diffusion / 4.0
    drift_z, drift_x, drift_y = speed_z / 4.0, speed_x / 4.0, speed_y / 4.0
    count_x, count_y = middle.shape
    plus_x = pltpu.roll(middle, count_x - 1, 0)
    minus_x = pltpu.roll(middle, 1, 0)
    plus_y = pltpu.roll(middle, count_y - 1, 1)
    minus_y = pltpu.roll(middle, 1, 1)
    return (
        (flow - drift_z) * upper_z
        + (flow + drift_z) * lower_z
        + (flow - drift_x) * plus_x
        + (flow + drift_x) * minus_x
        + (flow - drift_y) * plus_y
        + (flow + drift_y) * minus_y
        - 6.0 * flow * middle
        + rate_field * middle / (1.0 + middle * middle)
        + source_term
    )


def chain_kernel(
    count_t, count_s, detail, warm_c, rate_c, source_c,
    seed_detail, halo, start_out, first_out, second_out,
    start, rate_wide, source_wide, send_sem, recv_sem, seed_sem,
):
    rank, slab = lax.axis_index("tm"), lax.axis_index("space")
    last = count_t - 1
    layers, depth = warm_c.shape[0], detail.shape[0]
    above, below = slab < count_s - 1, slab > 0
    slab_up, slab_down = jnp.minimum(slab + 1, count_s - 1), jnp.maximum(slab - 1, 0)
    following = lax.rem(rank + 1, count_t)

    def copy(source, target, index, to_rank, to_slab):
        return pltpu.make_async_remote_copy(
            src_ref=source,
            dst_ref=target,
            send_sem=send_sem.at[index],
            recv_sem=recv_sem.at[index],
            device_id={"tm": to_rank, "space": to_slab},
            device_id_type=MESH,
        )

    def chain_copies(value):
        return (
            copy(value, start.at[0:layers], 6, following, slab_up),
            copy(value, start.at[layers : 2 * layers], 7, following, slab),
            copy(value, start.at[2 * layers : 3 * layers], 8, following, slab_down),
        )

    own_second = second_out.at[1 : layers + 1]
    chain_seed = chain_copies(warm_c)
    chain_next = chain_copies(own_second)
    ups = (
        copy(source_c.at[layers - 1 : layers], source_wide.at[0:1], 0, rank, slab_up),
        copy(rate_c.at[layers - 1 : layers], rate_wide.at[0:1], 1, rank, slab_up),
        copy(detail.at[depth - 1 : depth], halo.at[0:1], 2, rank, slab_up),
    )
    downs = (
        copy(source_c.at[0:1], source_wide.at[layers + 1 : layers + 2], 3, rank, slab_down),
        copy(rate_c.at[0:1], rate_wide.at[layers + 1 : layers + 2], 4, rank, slab_down),
        copy(detail.at[0:1], halo.at[1:2], 5, rank, slab_down),
    )
    edge_up = copy(second_out.at[layers : layers + 1], second_out.at[0:1], 9, rank, slab_up)
    edge_down = copy(second_out.at[1:2], second_out.at[layers + 1 : layers + 2], 10, rank, slab_down)

    targets = [last - 1] + list(range(last - 2, -1, -2))
    seeds, seed_halos = [], []
    for place, target in enumerate(targets):
        for kind, group, source, region in (
            (0, seeds, detail, seed_detail.at[0:depth]),
            (1, seed_halos, halo, seed_detail.at[depth : depth + 2]),
        ):
            group.append(
                pltpu.make_async_remote_copy(
                    src_ref=source,
                    dst_ref=region,
                    send_sem=seed_sem.at[kind, place],
                    recv_sem=recv_sem.at[11 + kind],
                    device_id={"tm": target, "space": slab},
                    device_id_type=MESH,
                )
            )
    partner = jnp.maximum(rank - 1, 0)
    passed = (
        copy(seed_detail.at[0:depth], seed_detail.at[0:depth], 11, partner, slab),
        copy(seed_detail.at[depth : depth + 2], seed_detail.at[depth : depth + 2], 12, partner, slab),
    )
    is_last = rank == last
    leader = (rank < last) & (lax.rem(last - rank, 2) == 0)

    def each(condition, copies, act):
        @pl.when(condition)
        def _():
            for item in copies:
                getattr(item, act)()

    each(is_last & above, chain_seed[0:1], "start")
    each(is_last, chain_seed[1:2], "start")
    each(is_last & below, chain_seed[2:3], "start")
    each(above, ups, "start")
    each(below, downs, "start")
    each(is_last, seeds, "start")

    source_wide[1 : layers + 1] = source_c[...]
    rate_wide[1 : layers + 1] = rate_c[...]

    @pl.when(jnp.logical_not(below))
    def _():
        for ref in (source_wide, rate_wide, halo, second_out):
            ref[0:1] = jnp.zeros((1,) + ref.shape[1:], jnp.float32)
        start[0:layers] = jnp.zeros((layers,) + start.shape[1:], jnp.float32)

    @pl.when(jnp.logical_not(above))
    def _():
        for ref in (source_wide, rate_wide, halo, second_out):
            end = ref.shape[0]
            ref[end - 1 : end] = jnp.zeros((1,) + ref.shape[1:], jnp.float32)
        start[2 * layers : 3 * layers] = jnp.zeros((layers,) + start.shape[1:], jnp.float32)

    each(below, ups, "wait_recv")
    each(above, downs, "wait_recv")
    each(is_last, seed_halos, "start")

    @pl.when(is_last)
    def _():
        @pl.loop(0, depth)
        def _(layer):
            seed_detail[layer] = detail[layer]

        @pl.loop(0, 2)
        def _(side):
            seed_detail[depth + side] = halo[side]

    each(below, chain_seed[0:1], "wait_recv")
    each(rank >= 0, chain_seed[1:2], "wait_recv")
    each(above, chain_seed[2:3], "wait_recv")

    for layer in range(layers + 2):
        at = layer + layers - 1
        middle = start[at]
        value = middle + 0.5 * coarse_tendency(
            middle, start[at + 1], start[at - 1], rate_wide[layer], source_wide[layer]
        )
        if layer == 0:
            value = jnp.where(below, value, 0.0)
        if layer == layers + 1:
            value = jnp.where(above, value, 0.0)
        first_out[layer] = value
    for layer in range(1, layers + 1):
        middle = first_out[layer]
        second_out[layer] = middle + 0.5 * coarse_tendency(
            middle, first_out[layer + 1], first_out[layer - 1], rate_wide[layer], source_wide[layer]
        )

    going = rank < last
    each(going, chain_next[1:2], "start")
    each(going & above, chain_next[0:1], "start")
    each(going & below, chain_next[2:3], "start")
    each(above, (edge_up,), "start")
    each(below, (edge_down,), "start")
    start_out[...] = start[layers - 1 : 2 * layers + 1]

    each(going, passed, "wait_recv")
    each(leader, passed, "start")
    each(below, (edge_up,), "wait_recv")
    each(above, (edge_down,), "wait_recv")
    each(above, ups + (edge_up,) + chain_next[0:1], "wait_send")
    each(below, downs + (edge_down,) + chain_next[2:3], "wait_send")
    each(rank >= 0, chain_next[1:2], "wait_send")
    each(is_last, seeds + seed_halos, "wait_send")
    each(leader, passed, "wait_send")


def run_chain(mesh, detail, warm_c, rate_c, source_c):
    count_t, count_s = mesh.shape["tm"], mesh.shape["space"]
    layers, across, along = warm_c.shape
    depth, fine_x, fine_y = detail.shape
    wide = jax.ShapeDtypeStruct((layers + 2, across, along), jnp.float32)
    vmem = pl.BlockSpec(memory_space=pltpu.VMEM)
    return pl.pallas_call(
        functools.partial(chain_kernel, count_t, count_s),
        out_shape=[
            jax.ShapeDtypeStruct((depth + 2, fine_x, fine_y), jnp.float32),
            jax.ShapeDtypeStruct((2, fine_x, fine_y), jnp.float32),
            wide, wide, wide,
        ],
        in_specs=[vmem] * 4,
        out_specs=[vmem] * 5,
        scratch_shapes=[
            pltpu.VMEM((3 * layers, across, along), jnp.float32),
            pltpu.VMEM((layers + 2, across, along), jnp.float32),
            pltpu.VMEM((layers + 2, across, along), jnp.float32),
            pltpu.SemaphoreType.DMA((13,)),
            pltpu.SemaphoreType.DMA((13,)),
            pltpu.SemaphoreType.DMA((2, count_t // 2)),
        ],
        compiler_params=pltpu.CompilerParams(has_side_effects=True),
    )(detail, warm_c, rate_c, source_c)


def edge_kernel(count_s, value, halo, send_sem, recv_sem):
    rank, slab = lax.axis_index("tm"), lax.axis_index("space")
    depth = value.shape[0]
    above, below = slab < count_s - 1, slab > 0
    slab_up, slab_down = jnp.minimum(slab + 1, count_s - 1), jnp.maximum(slab - 1, 0)
    barrier = pltpu.get_barrier_semaphore()

    def copy(source, target, index, to_slab):
        return pltpu.make_async_remote_copy(
            src_ref=source,
            dst_ref=target,
            send_sem=send_sem.at[index],
            recv_sem=recv_sem.at[index],
            device_id={"tm": rank, "space": to_slab},
            device_id_type=MESH,
        )

    up = copy(value.at[depth - 1 : depth], halo.at[0:1], 0, slab_up)
    down = copy(value.at[0:1], halo.at[1:2], 1, slab_down)
    for there, to_slab in ((above, slab_up), (below, slab_down)):
        @pl.when(there)
        def _():
            pl.semaphore_signal(
                barrier, inc=1, device_id={"tm": rank, "space": to_slab}, device_id_type=MESH
            )

    @pl.when(above & below)
    def _():
        pl.semaphore_wait(barrier, 2)

    @pl.when(above != below)
    def _():
        pl.semaphore_wait(barrier, 1)

    @pl.when(above)
    def _():
        up.start()

    @pl.when(below)
    def _():
        down.start()

    @pl.when(jnp.logical_not(below))
    def _():
        halo[0:1] = jnp.zeros((1,) + halo.shape[1:], jnp.float32)

    @pl.when(jnp.logical_not(above))
    def _():
        halo[1:2] = jnp.zeros((1,) + halo.shape[1:], jnp.float32)

    @pl.when(below)
    def _():
        up.wait_recv()
        down.wait_send()

    @pl.when(above)
    def _():
        down.wait_recv()
        up.wait_send()


def exchange_edges(mesh, value):
    vmem = pl.BlockSpec(memory_space=pltpu.VMEM)
    return pl.pallas_call(
        functools.partial(edge_kernel, mesh.shape["space"]),
        out_shape=jax.ShapeDtypeStruct((2,) + value.shape[1:], jnp.float32),
        in_specs=[vmem],
        out_specs=vmem,
        scratch_shapes=[pltpu.SemaphoreType.DMA((2,)), pltpu.SemaphoreType.DMA((2,))],
        compiler_params=pltpu.CompilerParams(collective_id=1, has_side_effects=True),
    )(value)


def wrap(value, halo):
    return jnp.concatenate([halo[0:1], value, halo[1:2]], axis=0)


def spread(wide):
    layers = wide.shape[0] - 2
    fine = jnp.repeat(inject(wide), 2, axis=0)
    return fine[1 : 2 * layers + 3]


def shards(mesh, previous_end, source, rate):
    warm = previous_end[0]
    own_source = source[0]
    depth = warm.shape[0]
    warm_c = restrict(warm)
    rate_c = restrict(rate)
    source_c = restrict(own_source)
    detail = warm - jnp.repeat(inject(warm_c), 2, axis=0)
    seed_detail, halo, start, first, second = run_chain(mesh, detail, warm_c, rate_c, source_c)
    wide_detail = wrap(detail, halo)
    wide_seed = wrap(seed_detail[:depth], seed_detail[depth:])
    guess0 = wide_seed + spread(start)
    guess1 = wide_detail + spread(first)
    guess2 = wide_detail + spread(second)
    image0 = tendency(guess0, rate, own_source, 1.0)
    image1 = tendency(guess1, rate, own_source, 1.0)
    image2 = tendency(guess2, rate, own_source, 1.0)
    node_one = guess0[1:-1] + (
        weights_one[0] * image0 + weights_one[1] * image1 + weights_one[2] * image2
    )
    padded_one = wrap(node_one, exchange_edges(mesh, node_one))
    again = tendency(padded_one, rate, own_source, 1.0)
    node_two = (
        node_one
        + 0.5 * (again - image1)
        + (weights_two[0] * image0 + weights_two[1] * image1 + weights_two[2] * image2)
    )
    return jnp.stack([node_one, node_two])[None]


def solution(mesh):
    placed = (P("tm", "space", None, None), P("tm", "space", None, None), P("space", None, None))
    return jax.shard_map(
        functools.partial(shards, mesh),
        mesh=mesh,
        in_specs=placed,
        out_specs=P("tm", None, "space", None, None),
        check_vma=False,
    )
```

```python
import functools

import jax
import jax.numpy as jnp
from jax import lax
from jax.experimental import pallas as pl
from jax.experimental.pallas import tpu as pltpu
from jax.sharding import PartitionSpec as P

diffusion = 0.1
speed_z = 0.4
speed_x = 0.3
speed_y = 0.2
weights_one = (5.0 / 24.0, 1.0 / 3.0, -1.0 / 24.0)
weights_two = (-1.0 / 24.0, 1.0 / 3.0, 5.0 / 24.0)


def pair_table(count):
    fine_index = jnp.arange(count, dtype=jnp.int32)[:, None]
    coarse_index = jnp.arange(count // 2, dtype=jnp.int32)[None, :]
    return (fine_index // 2 == coarse_index).astype(jnp.float32)


def restrict(field):
    count_z, count_x, count_y = field.shape[-3:]
    paired = field.reshape(field.shape[:-3] + (count_z // 2, 2, count_x, count_y))
    summed_z = paired[..., 0, :, :] + paired[..., 1, :, :]
    summed_y = jnp.einsum(
        "...xy,yb->...xb", summed_z, pair_table(count_y), precision=lax.Precision.HIGHEST
    )
    summed_x = jnp.einsum(
        "...xb,xa->...ab", summed_y, pair_table(count_x), precision=lax.Precision.HIGHEST
    )
    return 0.125 * summed_x


def inject(coarse):
    count_x, count_y = coarse.shape[-2:]
    along_y = jnp.einsum(
        "...ab,yb->...ay", coarse, pair_table(2 * count_y), precision=lax.Precision.HIGHEST
    )
    along_x = jnp.einsum(
        "...ay,xa->...xy", along_y, pair_table(2 * count_x), precision=lax.Precision.HIGHEST
    )
    return along_x


MESH = pl.DeviceIdType.MESH


def layer_tendency(middle, upper_z, lower_z, rate_field, source_term, spacing):
    flow, twice = diffusion / (spacing * spacing), 2.0 * spacing
    drift_z, drift_x, drift_y = speed_z / twice, speed_x / twice, speed_y / twice
    count_x, count_y = middle.shape
    plus_x = pltpu.roll(middle, count_x - 1, 0)
    minus_x = pltpu.roll(middle, 1, 0)
    plus_y = pltpu.roll(middle, count_y - 1, 1)
    minus_y = pltpu.roll(middle, 1, 1)
    return (
        (flow - drift_z) * upper_z
        + (flow + drift_z) * lower_z
        + (flow - drift_x) * plus_x
        + (flow + drift_x) * minus_x
        + (flow - drift_y) * plus_y
        + (flow + drift_y) * minus_y
        - 6.0 * flow * middle
        + rate_field * middle / (1.0 + middle * middle)
        + source_term
    )


def chain_kernel(
    count_t, count_s, detail, warm_c, rate_c, source_c,
    seed_detail, halo, start_out, first_out, second_out,
    start, rate_wide, source_wide, send_sem, recv_sem, seed_sem,
):
    rank, slab = lax.axis_index("tm"), lax.axis_index("space")
    last = count_t - 1
    layers, depth = warm_c.shape[0], detail.shape[0]
    above, below = slab < count_s - 1, slab > 0
    slab_up, slab_down = jnp.minimum(slab + 1, count_s - 1), jnp.maximum(slab - 1, 0)
    following = lax.rem(rank + 1, count_t)

    def copy(source, target, index, to_rank, to_slab):
        return pltpu.make_async_remote_copy(
            src_ref=source,
            dst_ref=target,
            send_sem=send_sem.at[index],
            recv_sem=recv_sem.at[index],
            device_id={"tm": to_rank, "space": to_slab},
            device_id_type=MESH,
        )

    def chain_copies(value):
        return (
            copy(value, start.at[0:layers], 6, following, slab_up),
            copy(value, start.at[layers : 2 * layers], 7, following, slab),
            copy(value, start.at[2 * layers : 3 * layers], 8, following, slab_down),
        )

    own_second = second_out.at[1 : layers + 1]
    chain_seed = chain_copies(warm_c)
    chain_next = chain_copies(own_second)
    ups = (
        copy(source_c.at[layers - 1 : layers], source_wide.at[0:1], 0, rank, slab_up),
        copy(rate_c.at[layers - 1 : layers], rate_wide.at[0:1], 1, rank, slab_up),
        copy(detail.at[depth - 1 : depth], halo.at[0:1], 2, rank, slab_up),
    )
    downs = (
        copy(source_c.at[0:1], source_wide.at[layers + 1 : layers + 2], 3, rank, slab_down),
        copy(rate_c.at[0:1], rate_wide.at[layers + 1 : layers + 2], 4, rank, slab_down),
        copy(detail.at[0:1], halo.at[1:2], 5, rank, slab_down),
    )
    edge_up = copy(second_out.at[layers : layers + 1], second_out.at[0:1], 9, rank, slab_up)
    edge_down = copy(second_out.at[1:2], second_out.at[layers + 1 : layers + 2], 10, rank, slab_down)

    targets = [last - 1] + list(range(last - 2, -1, -2))
    seeds, seed_halos = [], []
    for place, target in enumerate(targets):
        for kind, group, source, region in (
            (0, seeds, detail, seed_detail.at[0:depth]),
            (1, seed_halos, halo, seed_detail.at[depth : depth + 2]),
        ):
            group.append(
                pltpu.make_async_remote_copy(
                    src_ref=source,
                    dst_ref=region,
                    send_sem=seed_sem.at[kind, place],
                    recv_sem=recv_sem.at[11 + kind],
                    device_id={"tm": target, "space": slab},
                    device_id_type=MESH,
                )
            )
    partner = jnp.maximum(rank - 1, 0)
    passed = (
        copy(seed_detail.at[0:depth], seed_detail.at[0:depth], 11, partner, slab),
        copy(seed_detail.at[depth : depth + 2], seed_detail.at[depth : depth + 2], 12, partner, slab),
    )
    is_last = rank == last
    leader = (rank < last) & (lax.rem(last - rank, 2) == 0)

    def each(condition, copies, act):
        @pl.when(condition)
        def _():
            for item in copies:
                getattr(item, act)()

    each(is_last & above, chain_seed[0:1], "start")
    each(is_last, chain_seed[1:2], "start")
    each(is_last & below, chain_seed[2:3], "start")
    each(above, ups, "start")
    each(below, downs, "start")
    each(is_last, seeds, "start")

    source_wide[1 : layers + 1] = source_c[...]
    rate_wide[1 : layers + 1] = rate_c[...]

    @pl.when(jnp.logical_not(below))
    def _():
        for ref in (source_wide, rate_wide, halo, second_out):
            ref[0:1] = jnp.zeros((1,) + ref.shape[1:], jnp.float32)
        start[0:layers] = jnp.zeros((layers,) + start.shape[1:], jnp.float32)

    @pl.when(jnp.logical_not(above))
    def _():
        for ref in (source_wide, rate_wide, halo, second_out):
            end = ref.shape[0]
            ref[end - 1 : end] = jnp.zeros((1,) + ref.shape[1:], jnp.float32)
        start[2 * layers : 3 * layers] = jnp.zeros((layers,) + start.shape[1:], jnp.float32)

    each(below, ups, "wait_recv")
    each(above, downs, "wait_recv")
    each(is_last, seed_halos, "start")

    @pl.when(is_last)
    def _():
        @pl.loop(0, depth)
        def _(layer):
            seed_detail[layer] = detail[layer]

        @pl.loop(0, 2)
        def _(side):
            seed_detail[depth + side] = halo[side]

    each(below, chain_seed[0:1], "wait_recv")
    each(rank >= 0, chain_seed[1:2], "wait_recv")
    each(above, chain_seed[2:3], "wait_recv")

    for layer in range(layers + 2):
        at = layer + layers - 1
        middle = start[at]
        value = middle + 0.5 * layer_tendency(
            middle, start[at + 1], start[at - 1], rate_wide[layer], source_wide[layer], 2.0
        )
        if layer == 0:
            value = jnp.where(below, value, 0.0)
        if layer == layers + 1:
            value = jnp.where(above, value, 0.0)
        first_out[layer] = value
    for layer in range(1, layers + 1):
        middle = first_out[layer]
        second_out[layer] = middle + 0.5 * layer_tendency(
            middle, first_out[layer + 1], first_out[layer - 1], rate_wide[layer], source_wide[layer], 2.0
        )

    going = rank < last
    each(going, chain_next[1:2], "start")
    each(going & above, chain_next[0:1], "start")
    each(going & below, chain_next[2:3], "start")
    each(above, (edge_up,), "start")
    each(below, (edge_down,), "start")
    start_out[...] = start[layers - 1 : 2 * layers + 1]

    each(going, passed, "wait_recv")
    each(leader, passed, "start")
    each(below, (edge_up,), "wait_recv")
    each(above, (edge_down,), "wait_recv")
    each(above, ups + (edge_up,) + chain_next[0:1], "wait_send")
    each(below, downs + (edge_down,) + chain_next[2:3], "wait_send")
    each(rank >= 0, chain_next[1:2], "wait_send")
    each(is_last, seeds + seed_halos, "wait_send")
    each(leader, passed, "wait_send")


def run_chain(mesh, detail, warm_c, rate_c, source_c):
    count_t, count_s = mesh.shape["tm"], mesh.shape["space"]
    layers, across, along = warm_c.shape
    depth, fine_x, fine_y = detail.shape
    wide = jax.ShapeDtypeStruct((layers + 2, across, along), jnp.float32)
    vmem = pl.BlockSpec(memory_space=pltpu.VMEM)
    return pl.pallas_call(
        functools.partial(chain_kernel, count_t, count_s),
        out_shape=[
            jax.ShapeDtypeStruct((depth + 2, fine_x, fine_y), jnp.float32),
            jax.ShapeDtypeStruct((2, fine_x, fine_y), jnp.float32),
            wide, wide, wide,
        ],
        in_specs=[vmem] * 4,
        out_specs=[vmem] * 5,
        scratch_shapes=[
            pltpu.VMEM((3 * layers, across, along), jnp.float32),
            pltpu.VMEM((layers + 2, across, along), jnp.float32),
            pltpu.VMEM((layers + 2, across, along), jnp.float32),
            pltpu.SemaphoreType.DMA((13,)),
            pltpu.SemaphoreType.DMA((13,)),
            pltpu.SemaphoreType.DMA((2, count_t // 2)),
        ],
        compiler_params=pltpu.CompilerParams(has_side_effects=True),
    )(detail, warm_c, rate_c, source_c)


def sweep_kernel(
    count_s, detail, halo, seed_detail, start, first, second, rate, source,
    nodes, edges, send_sem, recv_sem,
):
    rank, slab = lax.axis_index("tm"), lax.axis_index("space")
    depth = detail.shape[0]
    above, below = slab < count_s - 1, slab > 0
    slab_up, slab_down = jnp.minimum(slab + 1, count_s - 1), jnp.maximum(slab - 1, 0)
    barrier = pltpu.get_barrier_semaphore()

    def copy(origin, target, index, to_slab):
        return pltpu.make_async_remote_copy(
            src_ref=origin,
            dst_ref=target,
            send_sem=send_sem.at[index],
            recv_sem=recv_sem.at[index],
            device_id={"tm": rank, "space": to_slab},
            device_id_type=MESH,
        )

    up = copy(nodes.at[0, depth - 1], edges.at[0], 0, slab_up)
    down = copy(nodes.at[0, 0], edges.at[1], 1, slab_down)
    for there, to_slab in ((above, slab_up), (below, slab_down)):
        @pl.when(there)
        def _():
            pl.semaphore_signal(
                barrier, inc=1, device_id={"tm": rank, "space": to_slab}, device_id_type=MESH
            )

    def guess(ref, ends, shift, coarse, layer):
        if layer < 0:
            base = ends[shift]
        elif layer == depth:
            base = ends[shift + 1]
        else:
            base = ref[layer]
        return base + coarse[layer // 2 + 1]

    def node_one(layer):
        own, images = None, []
        for ref, ends, shift, coarse in (
            (seed_detail, seed_detail, depth, start),
            (detail, halo, 0, first),
            (detail, halo, 0, second),
        ):
            middle = guess(ref, ends, shift, coarse, layer)
            own = middle if own is None else own
            images.append(
                layer_tendency(
                    middle,
                    guess(ref, ends, shift, coarse, layer + 1),
                    guess(ref, ends, shift, coarse, layer - 1),
                    rate[layer], source[layer], 1.0,
                )
            )
        value = own + (
            weights_one[0] * images[0] + weights_one[1] * images[1] + weights_one[2] * images[2]
        )
        nodes[0, layer] = value
        nodes[1, layer] = value + (
            weights_two[0] * images[0]
            + (weights_two[1] - 0.5) * images[1]
            + weights_two[2] * images[2]
        )

    def node_two(layer):
        upper = edges[1] if layer == depth - 1 else nodes[0, layer + 1]
        lower = edges[0] if layer == 0 else nodes[0, layer - 1]
        nodes[1, layer] += 0.5 * layer_tendency(
            nodes[0, layer], upper, lower, rate[layer], source[layer], 1.0
        )

    node_one(0)
    node_one(depth - 1)

    @pl.when(above & below)
    def _():
        pl.semaphore_wait(barrier, 2)

    @pl.when(above != below)
    def _():
        pl.semaphore_wait(barrier, 1)

    @pl.when(above)
    def _():
        up.start()

    @pl.when(below)
    def _():
        down.start()

    @pl.when(jnp.logical_not(below))
    def _():
        edges[0] = jnp.zeros(edges.shape[1:], jnp.float32)

    @pl.when(jnp.logical_not(above))
    def _():
        edges[1] = jnp.zeros(edges.shape[1:], jnp.float32)

    for layer in range(1, depth - 1):
        node_one(layer)
    for layer in range(1, depth - 1):
        node_two(layer)

    @pl.when(below)
    def _():
        up.wait_recv()
        down.wait_send()

    @pl.when(above)
    def _():
        down.wait_recv()
        up.wait_send()

    node_two(0)
    node_two(depth - 1)


def run_sweep(mesh, *operands):
    vmem = pl.BlockSpec(memory_space=pltpu.VMEM)
    shape = operands[0].shape
    return pl.pallas_call(
        functools.partial(sweep_kernel, mesh.shape["space"]),
        out_shape=jax.ShapeDtypeStruct((2,) + shape, jnp.float32),
        in_specs=[vmem] * len(operands),
        out_specs=vmem,
        scratch_shapes=[
            pltpu.VMEM((2,) + shape[1:], jnp.float32),
            pltpu.SemaphoreType.DMA((2,)),
            pltpu.SemaphoreType.DMA((2,)),
        ],
        compiler_params=pltpu.CompilerParams(collective_id=1, has_side_effects=True),
    )(*operands)


def shards(mesh, previous_end, source, rate):
    warm = previous_end[0]
    own_source = source[0]
    warm_c = restrict(warm)
    rate_c = restrict(rate)
    source_c = restrict(own_source)
    detail = warm - jnp.repeat(inject(warm_c), 2, axis=0)
    seed_detail, halo, start, first, second = run_chain(mesh, detail, warm_c, rate_c, source_c)
    return run_sweep(
        mesh, detail, halo, seed_detail,
        inject(start), inject(first), inject(second), rate, own_source,
    )[None]


def solution(mesh):
    placed = (P("tm", "space", None, None), P("tm", "space", None, None), P("space", None, None))
    return jax.shard_map(
        functools.partial(shards, mesh),
        mesh=mesh,
        in_specs=placed,
        out_specs=P("tm", None, "space", None, None),
        check_vma=False,
    )
```

```python
import functools

import jax
import jax.numpy as jnp
from jax import lax
from jax.experimental import pallas as pl
from jax.experimental.pallas import tpu as pltpu
from jax.sharding import PartitionSpec as P

diffusion = 0.1
speed_z = 0.4
speed_x = 0.3
speed_y = 0.2
weights_one = (5.0 / 24.0, 1.0 / 3.0, -1.0 / 24.0)
weights_two = (-1.0 / 24.0, 1.0 / 3.0, 5.0 / 24.0)


def pair_table(count):
    fine_index = jnp.arange(count, dtype=jnp.int32)[:, None]
    coarse_index = jnp.arange(count // 2, dtype=jnp.int32)[None, :]
    return (fine_index // 2 == coarse_index).astype(jnp.float32)


def restrict(field):
    count_z, count_x, count_y = field.shape[-3:]
    paired = field.reshape(field.shape[:-3] + (count_z // 2, 2, count_x, count_y))
    summed_z = paired[..., 0, :, :] + paired[..., 1, :, :]
    summed_y = jnp.einsum(
        "...xy,yb->...xb", summed_z, pair_table(count_y), precision=lax.Precision.HIGHEST
    )
    summed_x = jnp.einsum(
        "...xb,xa->...ab", summed_y, pair_table(count_x), precision=lax.Precision.HIGHEST
    )
    return 0.125 * summed_x


def inject(coarse):
    count_x, count_y = coarse.shape[-2:]
    along_y = jnp.einsum(
        "...ab,yb->...ay", coarse, pair_table(2 * count_y), precision=lax.Precision.HIGHEST
    )
    along_x = jnp.einsum(
        "...ay,xa->...xy", along_y, pair_table(2 * count_x), precision=lax.Precision.HIGHEST
    )
    return along_x


MESH = pl.DeviceIdType.MESH


def layer_tendency(middle, upper_z, lower_z, rate_field, source_term, spacing):
    flow, twice = diffusion / (spacing * spacing), 2.0 * spacing
    drift_z, drift_x, drift_y = speed_z / twice, speed_x / twice, speed_y / twice
    count_x, count_y = middle.shape
    plus_x = pltpu.roll(middle, count_x - 1, 0)
    minus_x = pltpu.roll(middle, 1, 0)
    plus_y = pltpu.roll(middle, count_y - 1, 1)
    minus_y = pltpu.roll(middle, 1, 1)
    return (
        (flow - drift_z) * upper_z
        + (flow + drift_z) * lower_z
        + (flow - drift_x) * plus_x
        + (flow + drift_x) * minus_x
        + (flow - drift_y) * plus_y
        + (flow + drift_y) * minus_y
        - 6.0 * flow * middle
        + rate_field * middle / (1.0 + middle * middle)
        + source_term
    )


def chain_kernel(
    count_t, count_s, detail, warm_c, rate_c, source_c,
    seed_detail, halo, start_out, first_out, second_out,
    start, rate_wide, source_wide, send_sem, recv_sem, seed_sem,
):
    rank, slab = lax.axis_index("tm"), lax.axis_index("space")
    last = count_t - 1
    layers, depth = warm_c.shape[0], detail.shape[0]
    above, below = slab < count_s - 1, slab > 0
    slab_up, slab_down = jnp.minimum(slab + 1, count_s - 1), jnp.maximum(slab - 1, 0)
    following = lax.rem(rank + 1, count_t)

    def copy(source, target, index, to_rank, to_slab):
        return pltpu.make_async_remote_copy(
            src_ref=source,
            dst_ref=target,
            send_sem=send_sem.at[index],
            recv_sem=recv_sem.at[index],
            device_id={"tm": to_rank, "space": to_slab},
            device_id_type=MESH,
        )

    def chain_copies(value):
        return (
            copy(value, start.at[0:layers], 6, following, slab_up),
            copy(value, start.at[layers : 2 * layers], 7, following, slab),
            copy(value, start.at[2 * layers : 3 * layers], 8, following, slab_down),
        )

    own_second = second_out.at[1 : layers + 1]
    chain_seed = chain_copies(warm_c)
    chain_next = chain_copies(own_second)
    ups = (
        copy(source_c.at[layers - 1 : layers], source_wide.at[0:1], 0, rank, slab_up),
        copy(rate_c.at[layers - 1 : layers], rate_wide.at[0:1], 1, rank, slab_up),
        copy(detail.at[depth - 1 : depth], halo.at[0:1], 2, rank, slab_up),
    )
    downs = (
        copy(source_c.at[0:1], source_wide.at[layers + 1 : layers + 2], 3, rank, slab_down),
        copy(rate_c.at[0:1], rate_wide.at[layers + 1 : layers + 2], 4, rank, slab_down),
        copy(detail.at[0:1], halo.at[1:2], 5, rank, slab_down),
    )
    edge_up = copy(second_out.at[layers : layers + 1], second_out.at[0:1], 9, rank, slab_up)
    edge_down = copy(second_out.at[1:2], second_out.at[layers + 1 : layers + 2], 10, rank, slab_down)

    targets = [last - 1] + list(range(last - 2, -1, -2))
    seeds, seed_halos = [], []
    for place, target in enumerate(targets):
        for kind, group, source, region in (
            (0, seeds, detail, seed_detail.at[0:depth]),
            (1, seed_halos, halo, seed_detail.at[depth : depth + 2]),
        ):
            group.append(
                pltpu.make_async_remote_copy(
                    src_ref=source,
                    dst_ref=region,
                    send_sem=seed_sem.at[kind, place],
                    recv_sem=recv_sem.at[11 + kind],
                    device_id={"tm": target, "space": slab},
                    device_id_type=MESH,
                )
            )
    partner = jnp.maximum(rank - 1, 0)
    passed = (
        copy(seed_detail.at[0:depth], seed_detail.at[0:depth], 11, partner, slab),
        copy(seed_detail.at[depth : depth + 2], seed_detail.at[depth : depth + 2], 12, partner, slab),
    )
    is_last = rank == last
    leader = (rank < last) & (lax.rem(last - rank, 2) == 0)

    def each(condition, copies, act):
        @pl.when(condition)
        def _():
            for item in copies:
                getattr(item, act)()

    each(is_last & above, chain_seed[0:1], "start")
    each(is_last, chain_seed[1:2], "start")
    each(is_last & below, chain_seed[2:3], "start")
    each(above, ups, "start")
    each(below, downs, "start")
    each(is_last, seeds, "start")

    source_wide[1 : layers + 1] = source_c[...]
    rate_wide[1 : layers + 1] = rate_c[...]

    @pl.when(jnp.logical_not(below))
    def _():
        for ref in (source_wide, rate_wide, halo, second_out):
            ref[0:1] = jnp.zeros((1,) + ref.shape[1:], jnp.float32)
        start[0:layers] = jnp.zeros((layers,) + start.shape[1:], jnp.float32)

    @pl.when(jnp.logical_not(above))
    def _():
        for ref in (source_wide, rate_wide, halo, second_out):
            end = ref.shape[0]
            ref[end - 1 : end] = jnp.zeros((1,) + ref.shape[1:], jnp.float32)
        start[2 * layers : 3 * layers] = jnp.zeros((layers,) + start.shape[1:], jnp.float32)

    each(below, ups[0:2], "wait_recv")
    each(above, downs[0:2], "wait_recv")
    each(is_last & below, ups[2:3], "wait_recv")
    each(is_last & above, downs[2:3], "wait_recv")
    each(is_last, seed_halos, "start")

    @pl.when(is_last)
    def _():
        @pl.loop(0, depth)
        def _(layer):
            seed_detail[layer] = detail[layer]

        @pl.loop(0, 2)
        def _(side):
            seed_detail[depth + side] = halo[side]

    each(below, chain_seed[0:1], "wait_recv")
    each(rank >= 0, chain_seed[1:2], "wait_recv")
    each(above, chain_seed[2:3], "wait_recv")

    for layer in range(layers + 2):
        at = layer + layers - 1
        middle = start[at]
        value = middle + 0.5 * layer_tendency(
            middle, start[at + 1], start[at - 1], rate_wide[layer], source_wide[layer], 2.0
        )
        if layer == 0:
            value = jnp.where(below, value, 0.0)
        if layer == layers + 1:
            value = jnp.where(above, value, 0.0)
        first_out[layer] = value
    for layer in range(1, layers + 1):
        middle = first_out[layer]
        second_out[layer] = middle + 0.5 * layer_tendency(
            middle, first_out[layer + 1], first_out[layer - 1], rate_wide[layer], source_wide[layer], 2.0
        )

    going = rank < last
    each(going & above, chain_next[0:1], "start")
    each(going & below, chain_next[2:3], "start")
    each(going, chain_next[1:2], "start")
    each(above, (edge_up,), "start")
    each(below, (edge_down,), "start")
    start_out[...] = start[layers - 1 : 2 * layers + 1]

    each(going & below, ups[2:3], "wait_recv")
    each(going & above, downs[2:3], "wait_recv")
    each(going, passed, "wait_recv")
    each(leader, passed, "start")
    each(below, (edge_up,), "wait_recv")
    each(above, (edge_down,), "wait_recv")
    each(above, ups + (edge_up,) + chain_next[0:1], "wait_send")
    each(below, downs + (edge_down,) + chain_next[2:3], "wait_send")
    each(rank >= 0, chain_next[1:2], "wait_send")
    each(is_last, seeds + seed_halos, "wait_send")
    each(leader, passed, "wait_send")


def run_chain(mesh, detail, warm_c, rate_c, source_c):
    count_t, count_s = mesh.shape["tm"], mesh.shape["space"]
    layers, across, along = warm_c.shape
    depth, fine_x, fine_y = detail.shape
    wide = jax.ShapeDtypeStruct((layers + 2, across, along), jnp.float32)
    vmem = pl.BlockSpec(memory_space=pltpu.VMEM)
    return pl.pallas_call(
        functools.partial(chain_kernel, count_t, count_s),
        out_shape=[
            jax.ShapeDtypeStruct((depth + 2, fine_x, fine_y), jnp.float32),
            jax.ShapeDtypeStruct((2, fine_x, fine_y), jnp.float32),
            wide, wide, wide,
        ],
        in_specs=[vmem] * 4,
        out_specs=[vmem] * 5,
        scratch_shapes=[
            pltpu.VMEM((3 * layers, across, along), jnp.float32),
            pltpu.VMEM((layers + 2, across, along), jnp.float32),
            pltpu.VMEM((layers + 2, across, along), jnp.float32),
            pltpu.SemaphoreType.DMA((13,)),
            pltpu.SemaphoreType.DMA((13,)),
            pltpu.SemaphoreType.DMA((2, count_t // 2)),
        ],
        compiler_params=pltpu.CompilerParams(has_side_effects=True),
    )(detail, warm_c, rate_c, source_c)


def sweep_kernel(
    count_s, detail, halo, seed_detail, start, first, second, rate, source,
    nodes, edges, send_sem, recv_sem,
):
    rank, slab = lax.axis_index("tm"), lax.axis_index("space")
    depth = detail.shape[0]
    above, below = slab < count_s - 1, slab > 0
    slab_up, slab_down = jnp.minimum(slab + 1, count_s - 1), jnp.maximum(slab - 1, 0)
    barrier = pltpu.get_barrier_semaphore()

    def copy(origin, target, index, to_slab):
        return pltpu.make_async_remote_copy(
            src_ref=origin,
            dst_ref=target,
            send_sem=send_sem.at[index],
            recv_sem=recv_sem.at[index],
            device_id={"tm": rank, "space": to_slab},
            device_id_type=MESH,
        )

    up = copy(nodes.at[0, depth - 1], edges.at[0], 0, slab_up)
    down = copy(nodes.at[0, 0], edges.at[1], 1, slab_down)
    for there, to_slab in ((above, slab_up), (below, slab_down)):
        @pl.when(there)
        def _():
            pl.semaphore_signal(
                barrier, inc=1, device_id={"tm": rank, "space": to_slab}, device_id_type=MESH
            )

    def guess(ref, ends, shift, coarse, layer):
        if layer < 0:
            base = ends[shift]
        elif layer == depth:
            base = ends[shift + 1]
        else:
            base = ref[layer]
        return base + coarse[layer // 2 + 1]

    def node_one(layer):
        own, images = None, []
        for ref, ends, shift, coarse in (
            (seed_detail, seed_detail, depth, start),
            (detail, halo, 0, first),
            (detail, halo, 0, second),
        ):
            middle = guess(ref, ends, shift, coarse, layer)
            own = middle if own is None else own
            images.append(
                layer_tendency(
                    middle,
                    guess(ref, ends, shift, coarse, layer + 1),
                    guess(ref, ends, shift, coarse, layer - 1),
                    rate[layer], source[layer], 1.0,
                )
            )
        value = own + (
            weights_one[0] * images[0] + weights_one[1] * images[1] + weights_one[2] * images[2]
        )
        nodes[0, layer] = value
        nodes[1, layer] = value + (
            weights_two[0] * images[0]
            + (weights_two[1] - 0.5) * images[1]
            + weights_two[2] * images[2]
        )

    def node_two(layer):
        upper = edges[1] if layer == depth - 1 else nodes[0, layer + 1]
        lower = edges[0] if layer == 0 else nodes[0, layer - 1]
        nodes[1, layer] += 0.5 * layer_tendency(
            nodes[0, layer], upper, lower, rate[layer], source[layer], 1.0
        )

    node_one(0)
    node_one(depth - 1)

    @pl.when(above & below)
    def _():
        pl.semaphore_wait(barrier, 2)

    @pl.when(above != below)
    def _():
        pl.semaphore_wait(barrier, 1)

    @pl.when(above)
    def _():
        up.start()

    @pl.when(below)
    def _():
        down.start()

    @pl.when(jnp.logical_not(below))
    def _():
        edges[0] = jnp.zeros(edges.shape[1:], jnp.float32)

    @pl.when(jnp.logical_not(above))
    def _():
        edges[1] = jnp.zeros(edges.shape[1:], jnp.float32)

    for layer in range(1, depth - 1):
        node_one(layer)
    for layer in range(1, depth - 1):
        node_two(layer)

    @pl.when(below)
    def _():
        up.wait_recv()
        down.wait_send()

    @pl.when(above)
    def _():
        down.wait_recv()
        up.wait_send()

    node_two(0)
    node_two(depth - 1)


def run_sweep(mesh, *operands):
    vmem = pl.BlockSpec(memory_space=pltpu.VMEM)
    shape = operands[0].shape
    return pl.pallas_call(
        functools.partial(sweep_kernel, mesh.shape["space"]),
        out_shape=jax.ShapeDtypeStruct((2,) + shape, jnp.float32),
        in_specs=[vmem] * len(operands),
        out_specs=vmem,
        scratch_shapes=[
            pltpu.VMEM((2,) + shape[1:], jnp.float32),
            pltpu.SemaphoreType.DMA((2,)),
            pltpu.SemaphoreType.DMA((2,)),
        ],
        compiler_params=pltpu.CompilerParams(collective_id=1, has_side_effects=True),
    )(*operands)


def shards(mesh, previous_end, source, rate):
    warm = previous_end[0]
    own_source = source[0]
    warm_c = restrict(warm)
    rate_c = restrict(rate)
    source_c = restrict(own_source)
    detail = warm - jnp.repeat(inject(warm_c), 2, axis=0)
    seed_detail, halo, start, first, second = run_chain(mesh, detail, warm_c, rate_c, source_c)
    return run_sweep(
        mesh, detail, halo, seed_detail,
        inject(start), inject(first), inject(second), rate, own_source,
    )[None]


def solution(mesh):
    placed = (P("tm", "space", None, None), P("tm", "space", None, None), P("space", None, None))
    return jax.shard_map(
        functools.partial(shards, mesh),
        mesh=mesh,
        in_specs=placed,
        out_specs=P("tm", None, "space", None, None),
        check_vma=False,
    )
```
